32 devices in a mesh: ctx: 16 (over z, y, x), head: 2 (over core).
Axes of the slice: x: 2, y: 2, z: 4, core: 2. Of those that a mesh axis runs over, the one named last changes fastest.
Arguments:
- queries: bfloat16 [4096, 2048], P('ctx', 'head'), may hold values from -160 to 160
- keys: bfloat16 [4096, 256], P('ctx', 'head'), may hold values from -6 to 6
- values: bfloat16 [4096, 256], P('ctx', 'head'), may hold values from -6 to 6
- gain: bfloat16 [2048], P('head'), may hold values from 0.099609375 to 1.8984375
- d_normed: bfloat16 [4096, 2048], P('ctx', 'head'), may hold values from -6 to 6
- lengths: int32 [16], replicated, may hold values from 1 to 704, 4096 in all
Outputs:
- normed: bfloat16 [4096, 2048], P('ctx', 'head')
- d_queries: bfloat16 [4096, 2048], P('ctx', 'head')
- d_keys: bfloat16 [4096, 256], P('ctx', 'head')
- d_values: bfloat16 [4096, 256], P('ctx', 'head')
The draws below stay inside these ranges and needn't reach their ends.
Inputs may be any that keep to these rules, and one draw needn't show every extreme that they name: document lengths in order along the sequence, summing to 4096; the longest is exactly 704.
All inputs are finite; a program needn't handle non-finite values.
Results may differ from the reference program's by a relative error of at most 0.0096.
Values may be sent and summed in bfloat16 or wider, within the bound.
No kernel may reach another device: no remote copies, remote signals or barrier semaphores. Data moves between devices by JAX's collectives and lax.ppermute only.
A program may use at most 64 MiB of HBM per device.

```python
import math
import jax
import jax.numpy as jnp
import numpy as np
from jax import lax

HD = 128
GROUP = 8
HOPS = 6
TOK_DEV = 256
KV_HEADS = 2
HEADS = 16
TOKENS = 4096
MAXDOC = 704
NDOCS = 16
N_CTX = 16


def query_key_pair(key):
    base = jax.random.fold_in(key, 911)
    first_key, second_key = jax.random.split(base)
    key_table = jnp.clip(jax.random.normal(first_key, (TOKENS, KV_HEADS, HD), jnp.float32), -6.0, 6.0)
    query_table = jnp.clip(jax.random.normal(second_key, (TOKENS, KV_HEADS, GROUP, HD), jnp.float32), -6.0, 6.0)
    return (query_table, key_table)


def draw_queries(key, part):
    query_table, key_table = query_key_pair(key)
    return query_table.reshape(TOKENS, HEADS * HD).astype(jnp.bfloat16)


def draw_keys(key, part):
    query_table, key_table = query_key_pair(key)
    return key_table.reshape(TOKENS, KV_HEADS * HD).astype(jnp.bfloat16)


def shard_levels(rng, shape, cuts, low, largest):
    loudness, own = 1.0, jax.random.fold_in(rng, 6)
    for dim, blocks in cuts:
        steps = jnp.exp(jax.random.uniform(jax.random.fold_in(own, dim), (blocks,), jnp.float32, low / len(cuts), largest / len(cuts)))
        loudness = loudness * jnp.repeat(steps, shape[dim] // blocks).reshape([-1 if axis == dim else 1 for axis in range(len(shape))])
    return loudness


def split_up(number_of, total, most, lean):
    portions = [(1 << 20) // math.isqrt(grade ** lean) + 1 for grade in range(2, number_of + 1)]
    spare, holding = total - most - (number_of - 1), [1] * (number_of - 1)
    while spare > 0:
        movable = [i for i in range(number_of - 1) if holding[i] < most]
        pool, left = sum([portions[i] for i in movable]), spare
        for i in movable:
            more = min(most - holding[i], max(1, left * portions[i] // pool), spare)
            holding[i] = holding[i] + more
            spare = spare - more
    return np.array([most] + holding)


def uneven(rng, amount, total, limit, slope):
    if amount == 2:
        one = jax.random.randint(rng, (), max(1, total - limit), min(limit, total - 1) + 1)
        return jnp.stack([one, total - one])
    sizes = jnp.asarray(split_up(amount, total, limit, slope), jnp.int32)
    twos = (amount - 1) // 2
    giver, receiver = sizes[1:1 + 2 * twos:2], sizes[2:2 + 2 * twos:2]
    slack = jnp.minimum(giver - 1, limit - receiver)
    moved = jax.random.randint(jax.random.fold_in(rng, 1), (twos,), 0, 1 << 20) % (slack + 1)
    sizes = sizes.at[1:1 + 2 * twos:2].set(giver - moved).at[2:2 + 2 * twos:2].set(receiver + moved)
    return sizes[jax.random.permutation(jax.random.fold_in(rng, 2), amount)]


def noise(key, extent, deviation, reach, pieces=(), held_as=jnp.bfloat16):
    drawn = jax.random.normal(key, extent, jnp.float32) * deviation
    if len(pieces) > 0:
        drawn = shard_levels(key, extent, pieces, -0.22, 0.18) * drawn
    return jnp.clip(drawn, min=-reach, max=reach).astype(held_as)


def setup_inputs(seed: int = 0) -> dict:
    key_of = jax.random.split(jax.random.key(seed), 7)
    return {
        "queries": draw_queries(jax.random.fold_in(key_of[6], 71), 0),
        "keys": draw_keys(jax.random.fold_in(key_of[6], 71), 0),
        "values": noise(key_of[2], (TOKENS, KV_HEADS * HD), 1.0, 6.0, ((0, 16), (1, 2))),
        "gain": jnp.clip(1.0 + 0.18 * jax.random.normal(key_of[3], (HEADS * HD,), jnp.float32), 0.099609375, 1.8984375).astype(jnp.bfloat16),
        "d_normed": noise(key_of[4], (TOKENS, HEADS * HD), 1.0, 6.0, ((0, 16), (1, 2))),
        "lengths": uneven(key_of[5], NDOCS, TOKENS, MAXDOC, 2).astype(jnp.int32),
    }


def document_ids(lengths):
    doc_ends = jnp.cumsum(lengths).astype(jnp.int32)
    marks = jnp.zeros((TOKENS + 1,), jnp.int32).at[doc_ends].add(1)
    return jnp.cumsum(marks[:TOKENS]).astype(jnp.int32)

def to_natural(array):
    stretch_rows = TOK_DEV // 2
    folded = array.reshape(N_CTX, 2, stretch_rows, array.shape[-1])
    return jnp.concatenate([folded[:, 0], folded[::-1, 1]], axis=0).reshape(TOKENS, array.shape[-1])

def from_natural(array):
    stretch_rows = TOK_DEV // 2
    stretches = array.reshape(2 * N_CTX, stretch_rows, array.shape[-1])
    lower = stretches[:N_CTX]
    upper = stretches[N_CTX:][::-1]
    return jnp.stack([lower, upper], axis=1).reshape(TOKENS, array.shape[-1])

def reference(queries, keys, values, gain, d_normed, lengths):
    stretch_rows = TOK_DEV // 2
    back = HOPS * stretch_rows
    window = back + stretch_rows
    count = 2 * N_CTX
    scale = HD ** (-0.5)
    width = HEADS * HD
    kv_width = KV_HEADS * HD
    docs = document_ids(lengths)
    doc_pad = jnp.concatenate([-jnp.ones((back,), jnp.int32), docs], axis=0)
    key_pad = jnp.concatenate([jnp.zeros((back, kv_width), keys.dtype), to_natural(keys)], axis=0)
    value_pad = jnp.concatenate([jnp.zeros((back, kv_width), values.dtype), to_natural(values)], axis=0)
    query_stretches = to_natural(queries).reshape(count, stretch_rows, width)
    grad_stretches = to_natural(d_normed).reshape(count, stretch_rows, width)
    gain_row = gain.astype(jnp.float32)

    def stretch_pass(carry, items):
        dk_pad, dv_pad = carry
        query_rows, grad_rows, index = items
        first = (index * stretch_rows).astype(jnp.int32)
        key_all = lax.dynamic_slice_in_dim(key_pad, first, window, 0).astype(jnp.float32).reshape(window, KV_HEADS, HD)
        value_all = lax.dynamic_slice_in_dim(value_pad, first, window, 0).astype(jnp.float32).reshape(window, KV_HEADS, HD)
        key_docs = lax.dynamic_slice_in_dim(doc_pad, first, window, 0)
        doc_rows = lax.dynamic_slice_in_dim(docs, first, stretch_rows, 0)
        query_pos = first + jnp.arange(stretch_rows, dtype=jnp.int32)
        key_pos = first - back + jnp.arange(window, dtype=jnp.int32)
        allowed = (key_docs[None, :] == doc_rows[:, None]) & (key_pos[None, :] <= query_pos[:, None]) & (key_pos[None, :] >= 0)
        query_four = query_rows.astype(jnp.float32).reshape(stretch_rows, KV_HEADS, GROUP, HD)
        scores = jnp.einsum('qkgd,skd->kgqs', query_four, key_all) * scale
        scores = jnp.where(allowed[None, None], scores, -1e+30)
        row_max = lax.optimization_barrier(jnp.max(scores, axis=-1, keepdims=True))
        expon = jnp.where(allowed[None, None], jnp.exp(scores - row_max), 0.0)
        weights = (expon / lax.optimization_barrier(jnp.sum(expon, axis=-1, keepdims=True))).astype(jnp.bfloat16)
        weight_f = weights.astype(jnp.float32)
        attended = jnp.einsum('kgqs,skd->qkgd', weight_f, value_all).reshape(stretch_rows, width).astype(jnp.bfloat16)
        attend_f = attended.astype(jnp.float32)
        factor = lax.rsqrt(lax.optimization_barrier(jnp.sum(attend_f * attend_f, axis=1)) / width + 1e-05)
        normed = (attend_f * factor[:, None] * gain_row[None, :]).astype(jnp.bfloat16)
        scaled_grad = grad_rows.astype(jnp.float32) * gain_row[None, :]
        inner = lax.optimization_barrier(jnp.sum(scaled_grad * attend_f, axis=1))
        d_attended = (factor[:, None] * (scaled_grad - attend_f * (factor * factor * inner / width)[:, None])).astype(jnp.bfloat16)
        d_att_four = d_attended.astype(jnp.float32).reshape(stretch_rows, KV_HEADS, GROUP, HD)
        att_four = attend_f.reshape(stretch_rows, KV_HEADS, GROUP, HD)
        delta = jnp.transpose(lax.optimization_barrier(jnp.sum(d_att_four * att_four, axis=-1)), (1, 2, 0))
        d_probs = jnp.einsum('qkgd,skd->kgqs', d_att_four, value_all)
        d_scores = (weight_f * (d_probs - delta[..., None])).astype(jnp.bfloat16).astype(jnp.float32)
        d_queries = (jnp.einsum('kgqs,skd->qkgd', d_scores, key_all) * scale).reshape(stretch_rows, width).astype(jnp.bfloat16)
        d_keys = (jnp.einsum('kgqs,qkgd->skd', d_scores, query_four) * scale).reshape(window, kv_width)
        d_values = jnp.einsum('kgqs,qkgd->skd', weight_f, d_att_four).reshape(window, kv_width)
        dk_pad = lax.dynamic_update_slice_in_dim(dk_pad, lax.dynamic_slice_in_dim(dk_pad, first, window, 0) + d_keys, first, 0)
        dv_pad = lax.dynamic_update_slice_in_dim(dv_pad, lax.dynamic_slice_in_dim(dv_pad, first, window, 0) + d_values, first, 0)
        return ((dk_pad, dv_pad), (normed, d_queries))
    start_carry = (jnp.zeros((TOKENS + back, kv_width), jnp.float32), jnp.zeros((TOKENS + back, kv_width), jnp.float32))
    indices = jnp.arange(count, dtype=jnp.int32)
    (dk_pad, dv_pad), (normed, d_queries) = lax.scan(stretch_pass, start_carry, (query_stretches, grad_stretches, indices))
    d_keys = dk_pad[back:].astype(jnp.bfloat16)
    d_values = dv_pad[back:].astype(jnp.bfloat16)
    return (from_natural(normed.reshape(TOKENS, width)), from_natural(d_queries.reshape(TOKENS, width)), from_natural(d_keys), from_natural(d_values))
```

```python
import functools
import jax
import jax.numpy as jnp
import numpy as np
from jax import lax
from jax.experimental import pallas as pl
from jax.experimental.pallas import tpu as pltpu
from jax.sharding import PartitionSpec as P

HD = 128
HOPS = 6
SQUARE = 4

NT = (((1,), (1,)), ((), ()))
NN = (((1,), (0,)), ((), ()))


class Plan:
    def __init__(self, block):
        self.block = block
        self.half = block // 2
        self.first = 5 * block
        self.region = 3 * block
        self.stack = self.first + 3 * self.region

    def base(self, name, odd, own=0):
        near, other = (2, 3) if odd else (3, 2)
        place = {"below": near, "above": other, "far": 4}
        return own if name == "own" else place[name] * self.block

    def slots(self, j, m):
        own = 0 if (j ^ m) > j else self.block
        if m == 1:
            names = [("own", 1), ("below", 1), ("above", 1)]
        elif m == 2:
            near, part = ("above", "below") if j < 2 else ("below", "above")
            names = [("own", 1), (near, 1), (part, 0), ("far", 0)]
        elif j in (0, 3):
            names = [("own", 1), ("above" if j == 0 else "below", 1), ("far", 1)]
        else:
            names = [("own", 1), ("below", 1), ("above", 1)]
        return own, names

    def pack_row(self, odd, j):
        row = []
        for m in (1, 2, 3):
            own, names = self.slots(j, m)
            for name, full in names:
                start = self.base(name, odd, own)
                row += [start, start + self.half] if full else [start + self.half]
        return row

    def key_row(self, odd, last, i):
        def place(j, name, d):
            late = self.half if d == HOPS else 0
            if j == i:
                return self.base(name, odd) + late
            m = i ^ j
            offset = self.first + (m - 1) * self.region
            for other, full in self.slots(j, m)[1]:
                if other == name:
                    return offset + late if full else offset
                offset += self.block if full else self.half
            raise KeyError(name)

        row = []
        for d in range(1, HOPS + 1):
            if d <= i:
                row.append(place(i - d, "own", d))
            elif d <= i + SQUARE:
                row.append(place(i - d + SQUARE, "below", d))
            else:
                row.append(place(i - d + 2 * SQUARE, "far", d))
        for d in range(1, HOPS + 1):
            if i + d < SQUARE:
                row.append(place(i + d, "own", d))
            elif i + d < 2 * SQUARE:
                row.append(place(i + d - SQUARE, "above", d))
            elif last:
                row.append(place(3 * SQUARE - 1 - i - d, "below", d))
            else:
                row.append(place(i + d - 2 * SQUARE, "far", d))
        return row

    def table(self):
        rows = []
        for odd, last in ((False, False), (True, False), (True, True)):
            for i in range(SQUARE):
                rows.append(self.pack_row(odd, i) + self.key_row(odd, last, i))
        return np.asarray(rows, np.int32)


def routes(count):
    groups = count // SQUARE
    dev = lambda g, j: SQUARE * g + j
    spots = range(SQUARE)
    near = [(dev(g, j), dev(g ^ 1, j)) for g in range(groups) for j in spots]
    other = [
        (dev(g, j), dev(g + 1 if g % 2 else g - 1, j)) for g in range(1, groups - 1) for j in spots
    ] + [(dev(groups - 1, j), dev(groups - 1, SQUARE - 1 - j)) for j in spots]
    far = (
        [(dev(g, j), dev(g + 2, j)) for g in range(groups - 2) for j in (2, 3)]
        + [(dev(g, j), dev(g - 2, j)) for g in range(2, groups) for j in (0, 1)]
        + [(dev(groups - 1, 3), dev(groups - 2, 0)), (dev(groups - 1, 2), dev(groups - 2, 1))]
    )
    return near, other, far


PACK = 18


def pack_kernel(plan, tab, pairs, near, other, far, x1, x2, x3, stack):
    b, h = plan.block, plan.half
    stack[: 2 * b] = pairs[...]
    stack[2 * b : 3 * b] = near[...]
    stack[3 * b : 4 * b] = other[...]
    stack[4 * b : 5 * b] = far[...]
    for m, out in enumerate((x1, x2, x3)):
        for piece in range(6):
            start = pl.multiple_of(tab[m * 6 + piece], h)
            out[piece * h : (piece + 1) * h] = stack[pl.ds(start, h)]


def forward_kernel(
    plan, heads, docs, tab, lens, pairs, near, other, far, x1, x2, x3, queries, d_normed, gain,
    weights, attended, inverse, key_set, value_set, query_t, stats,
    stack, bias, scores, stacked_q, values_one,
):
    b, h = plan.block, plan.half
    span = 7 * b
    stack[: 2 * b] = pairs[...]
    stack[2 * b : 3 * b] = near[...]
    stack[3 * b : 4 * b] = other[...]
    stack[4 * b : 5 * b] = far[...]
    for m, ref in enumerate((x1, x2, x3)):
        stack[plan.first + m * plan.region : plan.first + (m + 1) * plan.region] = ref[...]
    factor = HD ** (-0.5) * 1.4426950408889634
    lane = lax.broadcasted_iota(jnp.int32, (b, HD), 1)
    values_one[:, HD:] = jnp.ones((span, HD), jnp.bfloat16)
    for part in range(2):
        start = tab[PACK + 2 * HOPS + part]
        own = part * b
        key_set[part, :b] = stack[own : own + b, :HD]
        value_set[part, :b] = stack[own : own + b, HD:]
        for d in range(1, HOPS + 1):
            rows = h if d == HOPS else b
            place = pl.multiple_of(tab[PACK + part * HOPS + d - 1], h)
            block = stack[pl.ds(place, rows)]
            key_set[part, d * b : d * b + rows] = block[:, :HD]
            value_set[part, d * b : d * b + rows] = block[:, HD:]
        key_set[part, HOPS * b + h :] = jnp.zeros((b - h, HD), jnp.bfloat16)
        value_set[part, HOPS * b + h :] = jnp.zeros((b - h, HD), jnp.bfloat16)
        values_one[:, :HD] = value_set[part]
        query_pos = start + lax.broadcasted_iota(jnp.int32, (b, HD), 0)

        def find(n, carry):
            end, first = carry
            end = end + lens[n]
            return end, jnp.where(end <= query_pos, end, first)

        _, first = lax.fori_loop(0, docs, find, (jnp.int32(0), jnp.zeros((b, HD), jnp.int32)))
        for d in range(HOPS + 1):
            if d < HOPS:
                key_pos = start - d * b + lane
            else:
                key_pos = jnp.where(lane < h, start - d * b + h + lane, -1)
            allowed = (key_pos >= first) & (key_pos <= query_pos)
            bias[:, d * b : (d + 1) * b] = jnp.where(allowed, 0.0, -1e30)
        rows = slice(part * b, (part + 1) * b)
        for g in range(heads):
            head = queries[rows, g * HD : (g + 1) * HD]
            stacked_q[g * b : (g + 1) * b] = head
            query_t[part, :, g * b : (g + 1) * b] = head.T
        scores[...] = lax.dot_general(
            stacked_q[...], key_set[part], NT, preferred_element_type=jnp.float32
        )
        step = 32

        def soften(t, _):
            at = pl.multiple_of(t * step, step)
            mask_at = pl.multiple_of(lax.rem(at, b), step)
            raw = scores[pl.ds(at, step)] + bias[pl.ds(mask_at, step)]
            top = jnp.max(raw, axis=1, keepdims=True)
            weights[part, pl.ds(at, step)] = jnp.exp2((raw - top) * factor).astype(jnp.bfloat16)
            return 0

        lax.fori_loop(0, heads * b // step, soften, 0, unroll=2)
        squares = jnp.zeros((b, HD), jnp.float32)
        inner = jnp.zeros((b, HD), jnp.float32)
        for g in range(heads):
            at = slice(g * b, (g + 1) * b)
            mixed = lax.dot_general(
                weights[part, at], values_one[...], NN, preferred_element_type=jnp.float32
            )
            inv = 1.0 / mixed[:, HD:]
            result = (mixed[:, :HD] * inv).astype(jnp.bfloat16)
            attended[part, at] = result
            inverse[part, at] = inv
            result = result.astype(jnp.float32)
            cols = slice(g * HD, (g + 1) * HD)
            scaled = d_normed[rows, cols].astype(jnp.float32) * gain[:, cols].astype(jnp.float32)
            squares += result * result
            inner += scaled * result
        squares = jnp.sum(squares, axis=1, keepdims=True)
        inner = jnp.sum(inner, axis=1, keepdims=True)
        stats[rows] = jnp.where(lane < HD // 2, squares, inner)


def backward_kernel(
    plan, heads, full_width, tab, own_stats, peer_stats, weights, attended, inverse, key_set,
    value_set, query_t, d_normed, gain,
    normed, d_queries, g1, g2, g3, held,
    grads, stacked, stacked_t, d_probs, d_scores, deltas,
):
    b, h = plan.block, plan.half
    scale = HD ** (-0.5)
    grads[...] = jnp.zeros_like(grads)
    for part in range(2):
        rows = slice(part * b, (part + 1) * b)
        total = own_stats[rows] + peer_stats[rows]
        root = lax.rsqrt(total[:, :1] / full_width + 1e-05)
        coef = root * root * total[:, HD // 2 : HD // 2 + 1] / full_width
        for g in range(heads):
            at = slice(g * b, (g + 1) * b)
            cols = slice(g * HD, (g + 1) * HD)
            gain_row = gain[:, cols].astype(jnp.float32)
            result = attended[part, at].astype(jnp.float32)
            scaled = d_normed[rows, cols].astype(jnp.float32) * gain_row
            normed[rows, cols] = (result * root * gain_row).astype(jnp.bfloat16)
            d_att = root * (scaled - result * coef) * inverse[part, at]
            d_att = d_att.astype(jnp.bfloat16)
            stacked[at] = d_att
            stacked_t[:, at] = d_att.T
            delta = jnp.sum(d_att.astype(jnp.float32) * result, axis=1, keepdims=True)
            deltas[at] = jnp.broadcast_to(delta, (b, HD))
        d_probs[...] = lax.dot_general(
            stacked[...], value_set[part], NT, preferred_element_type=jnp.float32
        )
        step = 32

        def soften(t, _):
            at = pl.ds(pl.multiple_of(t * step, step), step)
            delta = deltas[at, :1]
            d_scores[at] = (
                weights[part, at].astype(jnp.float32) * (d_probs[at] - delta)
            ).astype(jnp.bfloat16)
            return 0

        lax.fori_loop(0, heads * b // step, soften, 0, unroll=2)
        d_values = lax.dot_general(
            stacked_t[...], weights[part], NN, preferred_element_type=jnp.float32
        )
        d_keys = scale * lax.dot_general(
            query_t[part], d_scores[...], NN, preferred_element_type=jnp.float32
        )
        for d in range(HOPS + 1):
            size = h if d == HOPS else b
            if d == 0:
                place = part * b
            else:
                place = pl.multiple_of(tab[PACK + part * HOPS + d - 1], h)
            cols = slice(d * b, (d + 1) * b)
            grads[pl.ds(place, size), :HD] += d_keys[:, cols].T[:size]
            grads[pl.ds(place, size), HD:] += d_values[:, cols].T[:size]
        for g in range(heads):
            d_q = scale * lax.dot_general(
                d_scores[g * b : (g + 1) * b], key_set[part], NN, preferred_element_type=jnp.float32
            )
            d_queries[rows, g * HD : (g + 1) * HD] = d_q.astype(jnp.bfloat16)
    for m, out in enumerate((g1, g2, g3)):
        out[...] = grads[plan.first + m * plan.region : plan.first + (m + 1) * plan.region].astype(
            jnp.bfloat16
        )
    held[...] = grads[: plan.first]


def unpack_kernel(plan, tab, held, g1, g2, g3, own, near, other, far, total):
    b, h = plan.block, plan.half
    total[...] = held[...]
    for m, ref in enumerate((g1, g2, g3)):
        for piece in range(6):
            start = pl.multiple_of(tab[m * 6 + piece], h)
            total[pl.ds(start, h)] += ref[piece * h : (piece + 1) * h].astype(jnp.float32)
    own[...] = total[: 2 * b]
    near[...] = total[2 * b : 3 * b].astype(jnp.bfloat16)
    other[...] = total[3 * b : 4 * b].astype(jnp.bfloat16)
    far[...] = total[4 * b : 5 * b].astype(jnp.bfloat16)


def finish_kernel(plan, tab, own, near, other, far, d_keys, d_values, total):
    total[...] = own[...]
    for k, ref in enumerate((near, other, far)):
        start = pl.multiple_of(tab[PACK + 2 * HOPS + 2 + k], plan.half)
        total[pl.ds(start, plan.block)] += ref[...].astype(jnp.float32)
    d_keys[...] = total[:, :HD].astype(jnp.bfloat16)
    d_values[...] = total[:, HD:].astype(jnp.bfloat16)


def call(kernel, outs, scratch, flops, moved, limit=None):
    vmem = pl.BlockSpec(memory_space=pltpu.VMEM)
    smem = pl.BlockSpec(memory_space=pltpu.SMEM)

    def run(scalars, arrays):
        return pl.pallas_call(
            kernel,
            out_shape=[jax.ShapeDtypeStruct(s, t) for s, t in outs],
            in_specs=[smem] * len(scalars) + [vmem] * len(arrays),
            out_specs=[vmem] * len(outs),
            scratch_shapes=[pltpu.VMEM(s, t) for s, t in scratch],
            cost_estimate=pl.CostEstimate(flops=flops, bytes_accessed=moved, transcendentals=0),
            compiler_params=pltpu.CompilerParams(vmem_limit_bytes=limit),
        )(*scalars, *arrays)

    return run


def per_device(queries, keys, values, gain, d_normed, lengths):
    bf, f32 = jnp.bfloat16, jnp.float32
    count = lax.axis_size("ctx")
    me = lax.axis_index("ctx")
    block = queries.shape[0] // 2
    width = queries.shape[1]
    heads = width // HD
    full_width = width * lax.axis_size("head")
    head_count = lax.axis_size("head")
    plan = Plan(block)
    group, spot = me // SQUARE, me % SQUARE
    odd = group % 2
    last = (group == count // SQUARE - 1).astype(jnp.int32)
    row = lax.dynamic_index_in_dim(
        jnp.asarray(plan.table()), (odd + last) * SQUARE + spot, 0, keepdims=False
    )
    send_at = jnp.stack([odd * block, (1 - odd) * block, jnp.where(spot < 2, block, 0)])
    starts = jnp.stack([me * block, (2 * count - 1 - me) * block])
    tab = jnp.concatenate([row, starts, send_at]).astype(jnp.int32)
    near_route, other_route, far_route = routes(count)
    back = [(d, s) for s, d in far_route]
    swap = lambda v, m: lax.ppermute(v, "ctx", [(r, r ^ m) for r in range(count)])

    pairs = jnp.concatenate([keys, values], axis=1)
    pick = lambda k: lax.dynamic_slice_in_dim(pairs, send_at[k], block, 0)
    near = lax.ppermute(pick(0), "ctx", near_route)
    other = lax.ppermute(pick(1), "ctx", other_route)
    far = lax.ppermute(pick(2), "ctx", far_route)
    wide = 2 * HD
    region = ((plan.region, wide), bf)
    sent = call(
        functools.partial(pack_kernel, plan), [region] * 3, [((plan.first, wide), bf)], 1000, 10**6
    )((tab,), (pairs, near, other, far))
    got = [swap(v, m + 1) for m, v in enumerate(sent)]

    span = 7 * block
    stack_rows = heads * block
    dots = 2 * 2 * stack_rows * span * HD
    gain2 = gain.reshape(1, width)
    saved = call(
        functools.partial(forward_kernel, plan, heads, lengths.shape[0]),
        [
            ((2, stack_rows, span), bf),
            ((2, stack_rows, HD), bf),
            ((2, stack_rows, HD), f32),
            ((2, span, HD), bf),
            ((2, span, HD), bf),
            ((2, HD, stack_rows), bf),
            ((2 * block, HD), f32),
        ],
        [
            ((plan.stack, wide), bf),
            ((block, span), f32),
            ((stack_rows, span), f32),
            ((stack_rows, HD), bf),
            ((span, wide), bf),
        ],
        2 * dots,
        10**7,
    )((tab, lengths), (pairs, near, other, far, *got, queries, d_normed, gain2))
    *saved, stats = saved
    if head_count == 2:
        peer = lax.ppermute(stats, "head", [(0, 1), (1, 0)])
    else:
        stats, peer = lax.psum(stats, "head"), jnp.zeros_like(stats)
    normed, d_queries, g1, g2, g3, held = call(
        functools.partial(backward_kernel, plan, heads, full_width),
        [
            ((2 * block, width), bf),
            ((2 * block, width), bf),
            region,
            region,
            region,
            ((plan.first, wide), f32),
        ],
        [
            ((plan.stack, wide), f32),
            ((stack_rows, HD), bf),
            ((HD, stack_rows), bf),
            ((stack_rows, span), f32),
            ((stack_rows, span), bf),
            ((stack_rows, HD), f32),
        ],
        4 * dots,
        10**7,
    )((tab,), (stats, peer, *saved, d_normed, gain2))
    back_got = [swap(v, m + 1) for m, v in enumerate((g1, g2, g3))]
    half_sum = ((block, wide), bf)
    own, near_g, other_g, far_g = call(
        functools.partial(unpack_kernel, plan),
        [((2 * block, wide), f32), half_sum, half_sum, half_sum],
        [((plan.first, wide), f32)],
        1000,
        10**6,
    )((tab,), (held, *back_got))
    reverse = lambda route: [(d, s) for s, d in route]
    near_g = lax.ppermute(near_g, "ctx", reverse(near_route))
    other_g = lax.ppermute(other_g, "ctx", reverse(other_route))
    far_g = lax.ppermute(far_g, "ctx", back)
    kv = ((2 * block, HD), bf)
    d_keys, d_values = call(
        functools.partial(finish_kernel, plan), [kv, kv], [((2 * block, wide), f32)], 1000, 10**6
    )((tab,), (own, near_g, other_g, far_g))
    return normed, d_queries, d_keys, d_values


def solution(mesh):
    split = P("ctx", "head")
    return jax.shard_map(
        per_device,
        mesh=mesh,
        in_specs=(split, split, split, P("head"), split, P()),
        out_specs=(split, split, split, split),
        check_vma=False,
    )
```
